16 devices in a mesh: dp: 2 (over z), sp: 8 (over y, x, core).
Axes of the slice: x: 2, y: 2, z: 2, core: 2. Of those that a mesh axis runs over, the one named last changes fastest.
Arguments:
- hidden: bfloat16 [16, 1024, 3072], P('dp', 'sp'), parts along dimension 0
- norm_w: bfloat16 [3072], replicated
- w_qkv: bfloat16 [3072, 5120], replicated
- w_out: bfloat16 [24, 128, 3072], replicated
- long_factor: float32 [64], replicated
- grad_out: bfloat16 [16, 1024, 3072], P('dp', 'sp'), parts along dimension 0
Outputs:
- output 1: bfloat16 [16, 1024, 3072], P('dp', 'sp'), parts along dimension 0
- output 2: bfloat16 [16, 1024, 3072], P('dp', 'sp'), parts along dimension 0
- output 3: float32 [6144, 5120], P('dp'), parts along dimension 0
- output 4: float32 [48, 128, 3072], P('dp'), parts along dimension 0
- output 5: float32 [6144], P('dp'), parts along dimension 0
There are 2 independent parts. The reference program is written for one: setup_inputs(seed, part) draws one part's arguments, and reference() takes and returns one part's arrays. A program takes and returns all parts, laid end to end along the dimension named above; an argument that names none is the same for every part.
All inputs are finite; a program needn't handle non-finite values.
Results may differ from the reference program's by a relative error of at most 0.0105145.
Values are sent between devices in bfloat16 or wider.
A program may use at most 1 GiB of HBM per device.

```python
import math
import jax
import jax.numpy as jnp
from jax import lax

N_BATCH = 8
SEQ_LEN = 1024
D_MODEL = 3072
N_HEADS = 24
N_KV_HEADS = 8
HEAD_DIM = 128
ROT_DIM = 128

Q_WIDTH = N_HEADS * HEAD_DIM
KV_WIDTH = N_KV_HEADS * HEAD_DIM
QKV_WIDTH = Q_WIDTH + 2 * KV_WIDTH
GROUP_SIZE = N_HEADS // N_KV_HEADS
HALF_ROT = ROT_DIM // 2
NORM_EPS = 1e-5
ROPE_BASE = 10000.0
ROPE_GAIN = math.sqrt(1.0 + math.log(32.0) / math.log(4096.0))
MASK_VALUE = -1e30


def setup_inputs(seed: int = 0, part: int = 0) -> dict:
    part_key = jax.random.fold_in(jax.random.key(seed), part)
    key_hidden, key_grad = jax.random.split(part_key, 2)
    key_norm, key_qkv, key_out, key_factor = jax.random.split(jax.random.key(seed + 1), 4)
    act_shape = (N_BATCH, SEQ_LEN, D_MODEL)
    hidden = jax.random.normal(key_hidden, act_shape, jnp.float32)
    grad_out = jax.random.normal(key_grad, act_shape, jnp.float32)
    norm_w = jax.random.uniform(key_norm, (D_MODEL,), jnp.float32, 0.5, 1.5)
    w_qkv = jax.random.normal(key_qkv, (D_MODEL, QKV_WIDTH), jnp.float32) * (D_MODEL ** -0.5)
    out_std = (SEQ_LEN / (64.0 * Q_WIDTH)) ** 0.5
    w_out = jax.random.normal(key_out, (N_HEADS, HEAD_DIM, D_MODEL), jnp.float32) * out_std
    long_factor = jnp.exp(jax.random.uniform(key_factor, (HALF_ROT,), jnp.float32, 0.0, math.log(48.0)))
    return {
        'hidden': hidden.astype(jnp.bfloat16),
        'norm_w': norm_w.astype(jnp.bfloat16),
        'w_qkv': w_qkv.astype(jnp.bfloat16),
        'w_out': w_out.astype(jnp.bfloat16),
        'long_factor': long_factor,
        'grad_out': grad_out.astype(jnp.bfloat16),
    }


def to_grid(values):
    return values.astype(jnp.bfloat16).astype(jnp.float32)


def rope_tables(long_factor):
    positions = jnp.arange(SEQ_LEN).astype(jnp.float32)
    exponent = jnp.arange(HALF_ROT).astype(jnp.float32) / HALF_ROT
    inv_freq = 1.0 / (long_factor.astype(jnp.float32) * jnp.power(ROPE_BASE, exponent))
    angles = positions[:, None] * inv_freq[None, :]
    return jnp.cos(angles) * ROPE_GAIN, jnp.sin(angles) * ROPE_GAIN


def rotate(head_vals, cos_t, sin_t):
    cos_b = cos_t[None, :, None, :]
    sin_b = sin_t[None, :, None, :]
    first_half = head_vals[..., :HALF_ROT]
    second_half = head_vals[..., HALF_ROT:ROT_DIM]
    return jnp.concatenate([first_half * cos_b - second_half * sin_b, second_half * cos_b + first_half * sin_b, head_vals[..., ROT_DIM:]], axis=-1)


def head_attention(q_head, k_head, v_head):
    causal = jnp.arange(SEQ_LEN)[:, None] >= jnp.arange(SEQ_LEN)[None, :]
    scores = jnp.einsum('bqe,bse->bqs', q_head, k_head) * (HEAD_DIM ** -0.5)
    prob_mat = to_grid(jax.nn.softmax(jnp.where(causal[None], scores, MASK_VALUE), axis=-1))
    return to_grid(jnp.einsum('bqs,bse->bqe', prob_mat, v_head))


def attention(queries, key_vals, value_vals):
    head_major = jnp.moveaxis(queries, 2, 0)
    kv_index = jnp.arange(N_HEADS) // GROUP_SIZE
    saved_head = jax.checkpoint(head_attention)

    def one_head(operand):
        q_head, kv_id = operand
        k_head = lax.dynamic_index_in_dim(key_vals, kv_id, axis=2, keepdims=False)
        v_head = lax.dynamic_index_in_dim(value_vals, kv_id, axis=2, keepdims=False)
        return saved_head(q_head, k_head, v_head)

    per_head = lax.map(one_head, (head_major, kv_index))
    return jnp.moveaxis(per_head, 0, 2)


def block_forward(hidden_f, gain, w_qkv_f, w_out_f, cos_t, sin_t):
    inv_rms = lax.rsqrt(jnp.mean(hidden_f * hidden_f, axis=-1, keepdims=True) + NORM_EPS)
    normed = to_grid(hidden_f * inv_rms * gain)
    fused_qkv = jnp.dot(normed.reshape(N_BATCH * SEQ_LEN, D_MODEL), w_qkv_f, preferred_element_type=jnp.float32)
    fused_qkv = fused_qkv.reshape(N_BATCH, SEQ_LEN, QKV_WIDTH)
    queries = fused_qkv[..., :Q_WIDTH].reshape(N_BATCH, SEQ_LEN, N_HEADS, HEAD_DIM)
    key_vals = fused_qkv[..., Q_WIDTH:Q_WIDTH + KV_WIDTH].reshape(N_BATCH, SEQ_LEN, N_KV_HEADS, HEAD_DIM)
    value_vals = fused_qkv[..., Q_WIDTH + KV_WIDTH:].reshape(N_BATCH, SEQ_LEN, N_KV_HEADS, HEAD_DIM)
    attn_out = attention(to_grid(rotate(queries, cos_t, sin_t)), to_grid(rotate(key_vals, cos_t, sin_t)), to_grid(value_vals))
    projected = jnp.dot(attn_out.reshape(N_BATCH * SEQ_LEN, Q_WIDTH), w_out_f.reshape(Q_WIDTH, D_MODEL), preferred_element_type=jnp.float32)
    return (hidden_f + projected.reshape(N_BATCH, SEQ_LEN, D_MODEL)).astype(jnp.bfloat16)


def reference(hidden, norm_w, w_qkv, w_out, long_factor, grad_out):
    cos_t, sin_t = rope_tables(long_factor)

    def forward(hidden_f, gain, w_qkv_f, w_out_f):
        return block_forward(hidden_f, gain, w_qkv_f, w_out_f, cos_t, sin_t)

    block_out, pullback = jax.vjp(forward, hidden.astype(jnp.float32), norm_w.astype(jnp.float32), w_qkv.astype(jnp.float32), w_out.astype(jnp.float32))
    grad_hidden, grad_norm_w, grad_w_qkv, grad_w_out = pullback(grad_out)
    return (block_out, grad_hidden.astype(jnp.bfloat16), grad_w_qkv, grad_w_out, grad_norm_w)
```

```python
import functools
import math

import jax
import jax.numpy as jnp
from jax import lax
from jax.experimental import pallas as pl
from jax.experimental.pallas import tpu as pltpu
from jax.sharding import PartitionSpec as P

NORM_EPS = 1e-5
ROPE_BASE = 10000.0
ROPE_GAIN = math.sqrt(1.0 + math.log(32.0) / math.log(4096.0))
MASK_VALUE = -1e30
LOG2E = 1.4426950408889634
HEAD_DIM = 128
ROW_BLOCK = 256
CHUNKS = (1, 1, 2, 2, 1, 1)


HBM_SPEC = pl.BlockSpec(memory_space=pltpu.HBM)

NT = (((1,), (1,)), ((), ()))
NN = (((1,), (0,)), ((), ()))
TN = (((0,), (0,)), ((), ()))


def mm(a, b, dims):
    return lax.dot_general(a, b, dims, preferred_element_type=jnp.float32)


def rope_tables(seq_len, long_factor):
    half_rot = long_factor.shape[0]
    exponent = jnp.arange(half_rot, dtype=jnp.float32) / half_rot
    inv_freq = 1.0 / (long_factor * jnp.power(ROPE_BASE, exponent))
    angles = jnp.arange(seq_len).astype(jnp.float32)[:, None] * inv_freq[None, :]
    cos_t, sin_t = jnp.cos(angles) * ROPE_GAIN, jnp.sin(angles) * ROPE_GAIN
    return jnp.concatenate([cos_t, cos_t], axis=1), jnp.concatenate([-sin_t, sin_t], axis=1)


def attention_kernel(n_deps, q_ref, k_ref, v_ref, do_ref, cos_ref, sin_ref, *rest):
    o_ref, dq_ref, dk_ref, dv_ref, kb, vb, dk_acc, dv_acc = rest[n_deps:]
    head = pl.program_id(1)
    seq_len = q_ref.shape[0]
    half = HEAD_DIM // 2
    scale = HEAD_DIM ** -0.5
    cos_t, sin_t = cos_ref[...], sin_ref[...]

    @pl.when(head == 0)
    def _():
        k_raw = k_ref[...]
        kb[...] = (k_raw * cos_t + pltpu.roll(k_raw, half, 1) * sin_t).astype(jnp.bfloat16)
        vb[...] = v_ref[...].astype(jnp.bfloat16)
        dk_acc[...] = jnp.zeros_like(dk_acc)
        dv_acc[...] = jnp.zeros_like(dv_acc)

    row_id = lax.broadcasted_iota(jnp.int32, (ROW_BLOCK, ROW_BLOCK), 0)
    col_id = lax.broadcasted_iota(jnp.int32, (ROW_BLOCK, ROW_BLOCK), 1)
    causal = row_id >= col_id
    for i in range(seq_len // ROW_BLOCK):
        rows = pl.ds(i * ROW_BLOCK, ROW_BLOCK)
        q_raw = q_ref[rows, :]
        cos_i, sin_i = cos_ref[rows, :], sin_ref[rows, :]
        q_i = (q_raw * cos_i + pltpu.roll(q_raw, half, 1) * sin_i).astype(jnp.bfloat16)
        do_i = do_ref[rows, :]
        spans = [(i * ROW_BLOCK, ROW_BLOCK)]
        if i > 0:
            spans.append((0, i * ROW_BLOCK))
        scores = []
        for begin, width in spans:
            s = mm(q_i, kb[pl.ds(begin, width), :], NT)
            scores.append(jnp.where(causal, s, MASK_VALUE) if begin == i * ROW_BLOCK else s)
        top = jnp.max(scores[0], axis=-1, keepdims=True)
        for s in scores[1:]:
            top = jnp.maximum(top, jnp.max(s, axis=-1, keepdims=True))
        exps = [jnp.exp2((s - top) * (scale * LOG2E)) for s in scores]
        total = sum(jnp.sum(e, axis=-1, keepdims=True) for e in exps)
        inv_total = 1.0 / total
        probs = [e * inv_total for e in exps]
        probs_b = [p.astype(jnp.bfloat16) for p in probs]
        o_i = sum(mm(pb, vb[pl.ds(b, w), :], NN) for pb, (b, w) in zip(probs_b, spans))
        o_ref[rows, :] = o_i.astype(jnp.bfloat16)
        delta = jnp.sum(o_i * do_i.astype(jnp.float32), axis=-1, keepdims=True)
        dq_i = 0.0
        for p, pb, (begin, width) in zip(probs, probs_b, spans):
            cols = pl.ds(begin, width)
            dp = mm(do_i, vb[cols, :], NT)
            ds = (p * (dp - delta)).astype(jnp.bfloat16)
            dq_i = dq_i + mm(ds, kb[cols, :], NN)
            dk_acc[:, cols] += mm(q_i, ds, TN)
            dv_acc[:, cols] += mm(do_i, pb, TN)
        dq_i = dq_i * scale
        dq_ref[rows, :] = (dq_i * cos_i - pltpu.roll(dq_i, half, 1) * sin_i).astype(jnp.bfloat16)

    @pl.when(head == pl.num_programs(1) - 1)
    def _():
        dk = dk_acc[...].T * scale
        dk_ref[...] = (dk * cos_t - pltpu.roll(dk, half, 1) * sin_t).astype(jnp.bfloat16)
        dv_ref[...] = dv_acc[...].T.astype(jnp.bfloat16)


def attention(fused, grad_attn, cos_t, sin_t, first_kv, n_kv, group, n_heads, kv_heads, deps):
    seq_len = fused.shape[0]
    hd = HEAD_DIM
    block = (seq_len, hd)
    table = pl.BlockSpec(block, lambda g, h: (0, 0))
    per_q = pl.BlockSpec(block, lambda g, h: (0, g * group + h))
    per_kv = pl.BlockSpec(block, lambda g, h: (0, g))
    q_first = first_kv * group
    pairs = n_kv * group * seq_len * seq_len
    return pl.pallas_call(
        functools.partial(attention_kernel, len(deps)),
        grid=(n_kv, group),
        in_specs=[
            pl.BlockSpec(block, lambda g, h: (0, q_first + g * group + h)),
            pl.BlockSpec(block, lambda g, h: (0, n_heads + first_kv + g)),
            pl.BlockSpec(block, lambda g, h: (0, n_heads + kv_heads + first_kv + g)),
            per_q,
            table, table,
        ] + [HBM_SPEC] * len(deps),
        out_specs=[per_q, per_q, per_kv, per_kv],
        out_shape=[jax.ShapeDtypeStruct((seq_len, n_kv * group * hd), jnp.bfloat16)] * 2
        + [jax.ShapeDtypeStruct((seq_len, n_kv * hd), jnp.bfloat16)] * 2,
        scratch_shapes=[
            pltpu.VMEM(block, jnp.bfloat16), pltpu.VMEM(block, jnp.bfloat16),
            pltpu.VMEM((hd, seq_len), jnp.float32), pltpu.VMEM((hd, seq_len), jnp.float32),
        ],
        compiler_params=pltpu.CompilerParams(
            dimension_semantics=("arbitrary", "arbitrary"), vmem_limit_bytes=48 * 2 ** 20),
        cost_estimate=pl.CostEstimate(
            flops=16 * hd * pairs, transcendentals=pairs, bytes_accessed=n_kv * group * seq_len * hd * 12),
        name="attention",
    )(fused, fused, fused, grad_attn, cos_t, sin_t, *deps)


class Exchange:
    def __init__(self, n_dev):
        me = lax.axis_index('sp')
        core = me % 2
        bit_x, bit_y = (me // 2) % 2, me // 4
        b1, b2 = jnp.where(core == 0, bit_x, bit_y), jnp.where(core == 0, bit_y, bit_x)
        half, quarter = core * 4, core * 4 + b1 * 2
        other = (1 - core) * 4 + b2 * 2 + b1
        self.where = jnp.stack([4 - half, half + 2 - b1 * 2, quarter + 1 - b2, quarter + b2, half, quarter, other])
        self.where = self.where.astype(jnp.int32)
        flips = ((1, 1), (2, 4), (4, 2))
        self.perms = [[(d, d ^ flip[d % 2]) for d in range(n_dev)] for flip in flips]

    def send(self, values, level):
        return lax.ppermute(values, 'sp', self.perms[level])


def after(value, dep):
    return lax.optimization_barrier((value, dep))


def partial_kernel(n_arrived, where_ref, normed_ref, dy_ref, dq_ref, dk_ref, dv_ref, o_ref, *rest):
    arrived, out_ref = rest[:n_arrived], rest[-1]
    normed_t, dy_t = normed_ref[...], dy_ref[...]
    begin = 0
    for lhs, rhs_ref in ((normed_t, dq_ref), (normed_t, dk_ref), (normed_t, dv_ref), (dy_t, o_ref)):
        width = rhs_ref.shape[1]
        cols = pl.ds(begin, width)
        term = mm(lhs, rhs_ref[...], NN)
        for r in arrived:
            term = term + r[:, cols].astype(jnp.float32)
        out_ref[:, cols] = term.astype(jnp.bfloat16)
        begin += width


def partial_sum(level, where, normed_t, dy_t, grads, arrived, deps):
    d_model, seq_len = normed_t.shape
    rows = d_model // 8
    n_pieces = (4, 2, 1, 1)[level]
    width = sum(a.shape[1] for a in grads)
    lhs = pl.BlockSpec((rows, seq_len), lambda j, w: (w[level] + j, 0))
    offsets = (lambda j, w: (w[level] - w[4] + j, 0), lambda j, w: (w[level] - w[5] + j, 0), lambda j, w: (0, 0))
    return pl.pallas_call(
        functools.partial(partial_kernel, len(arrived)),
        grid_spec=pltpu.PrefetchScalarGridSpec(
            num_scalar_prefetch=1, grid=(n_pieces,),
            in_specs=[lhs, lhs] + [pl.BlockSpec(a.shape, lambda j, w: (0, 0)) for a in grads]
            + [pl.BlockSpec((rows, width), offsets[i]) for i in range(len(arrived))] + [HBM_SPEC] * len(deps),
            out_specs=pl.BlockSpec((rows, width), lambda j, w: (j, 0))),
        out_shape=jax.ShapeDtypeStruct((n_pieces * rows, width), jnp.bfloat16),
        compiler_params=pltpu.CompilerParams(dimension_semantics=("arbitrary",), vmem_limit_bytes=56 * 2 ** 20),
        cost_estimate=pl.CostEstimate(
            flops=2 * seq_len * rows * n_pieces * width, transcendentals=0,
            bytes_accessed=2 * (n_pieces * rows * (width * (1 + len(arrived)) + 2 * seq_len) + seq_len * width)),
        name="partial",
    )(where, normed_t, dy_t, *grads, *arrived, *deps)


def place_kernel(first_kv, n_kv, group, q_width, kv_width, n_extra, where_ref, *rest):
    pieces = rest[:8]
    wqkv_ref, wout_ref, token_ref, qkv_buf, out_buf, sems = rest[8 + n_extra:]
    token_ref[...] = jnp.zeros_like(token_ref)
    rows = pieces[0].shape[0]
    hd = HEAD_DIM
    wq, wk = n_kv * group * hd, n_kv * hd
    cols = (first_kv * group * hd, q_width + first_kv * hd, q_width + kv_width + first_kv * hd)
    flying = {}
    for j in range(8):
        slot = j % 2
        for copy in flying.get(slot, ()):
            copy.wait()
        index = (where_ref[3] if j < 4 else where_ref[6]) ^ (j % 4)
        begin = pl.multiple_of(index * rows, rows)
        qkv_buf[slot] = pieces[j][:, :wq + 2 * wk].astype(jnp.float32)
        out_buf[slot] = pieces[j][:, wq + 2 * wk:].astype(jnp.float32).T
        copies, at = [], 0
        for i, (width, col) in enumerate(zip((wq, wk, wk), cols)):
            copies.append(pltpu.make_async_copy(
                qkv_buf.at[slot, :, pl.ds(at, width)],
                wqkv_ref.at[pl.ds(begin, rows), pl.ds(col, width)], sems.at[slot, i]))
            at += width
        copies.append(pltpu.make_async_copy(
            out_buf.at[slot], wout_ref.at[pl.ds(first_kv * group * hd, wq), pl.ds(begin, rows)], sems.at[slot, 3]))
        for copy in copies:
            copy.start()
        flying[slot] = copies
    for slot in range(2):
        for copy in flying[slot]:
            copy.wait()


def place(where, pieces, sums, first_kv, n_kv, group, n_heads, kv_heads, deps):
    rows, width = pieces[0].shape
    hd = HEAD_DIM
    wq, wk = n_kv * group * hd, n_kv * hd
    d_model = 8 * rows
    shapes = [jax.ShapeDtypeStruct((d_model, (n_heads + 2 * kv_heads) * hd), jnp.float32),
              jax.ShapeDtypeStruct((n_heads * hd, d_model), jnp.float32),
              jax.ShapeDtypeStruct((8, hd), jnp.float32)]
    return pl.pallas_call(
        functools.partial(place_kernel, first_kv, n_kv, group, n_heads * hd, kv_heads * hd, len(sums) + len(deps)),
        in_specs=[pl.BlockSpec(memory_space=pltpu.SMEM)] + [pl.BlockSpec(memory_space=pltpu.VMEM)] * 8 + [HBM_SPEC] * (len(sums) + len(deps)),
        out_specs=[HBM_SPEC, HBM_SPEC, pl.BlockSpec(memory_space=pltpu.VMEM)],
        out_shape=shapes,
        input_output_aliases={9 + i: i for i in range(len(sums))},
        scratch_shapes=[pltpu.VMEM((2, rows, wq + 2 * wk), jnp.float32), pltpu.VMEM((2, wq, rows), jnp.float32),
                        pltpu.SemaphoreType.DMA((2, 4))],
        compiler_params=pltpu.CompilerParams(vmem_limit_bytes=48 * 2 ** 20),
        cost_estimate=pl.CostEstimate(flops=rows * width * 8 * 200, transcendentals=0, bytes_accessed=rows * width * 8 * 6),
        name="place",
    )(where, *pieces, *sums, *deps)


def solution(mesh):
    n_dev = mesh.shape['sp']
    exchange_rows = functools.partial(lax.all_to_all, axis_name='sp', split_axis=0, concat_axis=0, tiled=True)
    to_sequence = functools.partial(lax.all_to_all, axis_name='sp', split_axis=0, concat_axis=1, tiled=True)

    def device_step(hidden, norm_w, w_qkv, w_out, long_factor, grad_out):
        n_heads, head_dim, d_model = w_out.shape
        kv_heads = (w_qkv.shape[1] // head_dim - n_heads) // 2
        group = n_heads // kv_heads
        seq_len = hidden.shape[1] * n_dev
        w_out2 = w_out.reshape(n_heads * head_dim, d_model)
        gain = norm_w.astype(jnp.float32)
        ex = Exchange(n_dev)
        cos_t, sin_t = rope_tables(seq_len, long_factor)

        x = to_sequence(hidden).reshape(seq_len, d_model)
        dy = to_sequence(grad_out).reshape(seq_len, d_model)

        x_f = x.astype(jnp.float32)
        inv_rms = lax.rsqrt(jnp.mean(x_f * x_f, axis=-1, keepdims=True) + NORM_EPS)
        normed = (x_f * inv_rms * gain).astype(jnp.bfloat16)
        fused = mm(normed, w_qkv, NN)

        n_chunks = len(CHUNKS)
        firsts = [sum(CHUNKS[:c]) for c in range(n_chunks)]
        grads, arrived, pieces = [], [[] for _ in range(n_chunks)], {}
        sums = []
        normed_t, dy_t = normed.T, dy.T
        last = ()

        def partial(level, c):
            nonlocal last
            if not 0 <= c < n_chunks:
                return
            out = partial_sum(level, ex.where, normed_t, dy_t, grads[c], arrived[c], last)
            if level < 3:
                arrived[c].append(ex.send(out, level))
            else:
                pieces[c] = [out]
                spread(2, c)
            last = (out,)

        def spread(level, c):
            if 0 <= c < n_chunks:
                pieces[c] = pieces[c] + [ex.send(p, level) for p in pieces[c]]

        def collect(slot):
            nonlocal sums, last
            last = last + tuple(p for c in (slot - 2, slot - 3) if 0 <= c < n_chunks for p in pieces[c][len(pieces[c]) // 2:])
            spread(1, slot - 2)
            spread(0, slot - 3)
            c = slot - 4
            if 0 <= c < n_chunks:
                *sums, token = place(ex.where, pieces[c], sums, firsts[c], CHUNKS[c], group, n_heads, kv_heads, last)
                last = (token,)

        for c in range(n_chunks):
            n_kv, q0 = CHUNKS[c], firsts[c] * group * head_dim
            w_c = w_out2[q0:q0 + n_kv * group * head_dim]
            do_c = mm(dy, w_c, NT).astype(jnp.bfloat16)
            if last:
                do_c, last = after(do_c, last)
            partial(1, c - 1)
            partial(3, c - 2)
            o_c, dq_c, dk_c, dv_c = attention(
                fused, do_c, cos_t, sin_t, firsts[c], n_kv, group, n_heads, kv_heads, last)
            grads.append((dq_c, dk_c, dv_c, o_c))
            last = (o_c,)
            partial(2, c - 1)
            partial(0, c)
            collect(c)

        attn = jnp.concatenate([g[3] for g in grads], axis=1)
        partial(1, n_chunks - 1)
        partial(3, n_chunks - 2)
        attn, last = after(attn, last)
        y = (x.astype(jnp.float32) + mm(attn, w_out2, NN)).astype(jnp.bfloat16)
        block_out = exchange_rows(y.reshape(n_dev, seq_len // n_dev, d_model))
        last = last + (y,)
        partial(2, n_chunks - 1)
        collect(n_chunks)

        grad_fused = jnp.concatenate([g[0] for g in grads] + [g[1] for g in grads] + [g[2] for g in grads], axis=1)
        partial(3, n_chunks - 1)
        grad_fused, last = after(grad_fused, last)
        grad_normed = mm(grad_fused, w_qkv, NT)
        unit = x.astype(jnp.float32) * inv_rms
        grad_norm_w = jnp.sum(grad_normed * unit, axis=0)
        grad_unit = grad_normed * gain
        mean_dot = jnp.mean(grad_unit * unit, axis=-1, keepdims=True)
        grad_x = (dy.astype(jnp.float32) + inv_rms * (grad_unit - unit * mean_dot)).astype(jnp.bfloat16)
        grad_hidden = exchange_rows(grad_x.reshape(n_dev, seq_len // n_dev, d_model))
        last = last + (grad_x,)
        for level in range(3):
            grad_norm_w = grad_norm_w + ex.send(grad_norm_w, level)
        for slot in range(n_chunks + 1, n_chunks + 4):
            collect(slot)
        grad_w_qkv, grad_w_out = sums
        return block_out, grad_hidden, grad_w_qkv, grad_w_out.reshape(n_heads, head_dim, d_model), grad_norm_w

    tok_spec = P('dp', 'sp', None)
    return jax.shard_map(device_step, mesh=mesh,
                         in_specs=(tok_spec, P(), P(), P(), P(), tok_spec),
                         out_specs=(tok_spec, tok_spec, P('dp', None), P('dp', None, None), P('dp')),
                         check_vma=False)
```
